32 devices in a mesh: dom: 4 (over y, core), rep: 8 (over z, x).
Axes of the slice: x: 2, y: 2, z: 4, core: 2. Of those that a mesh axis runs over, the one named last changes fastest.
Arguments:
- facts: float32 [131072, 256], P(('dom', 'rep')), may hold values from -6 to 6
- row_owner: int32 [131072, 1], P(('dom', 'rep')), may hold values from 0 to 3; in each aligned block of 4096 rows (0 to 4095, 4096 to 8191, ...) at most 2048 rows name the same one
- key_offset: int32 [131072], P(('dom', 'rep')), may hold values from 0 to 1023
Outputs:
- key_means: float32 [4096, 256], P(('dom', 'rep'))
- key_counts: float32 [4096], P(('dom', 'rep'))
The draws below stay inside these ranges and needn't reach their ends.
Inputs may be any that keep to these rules, and one draw needn't show every extreme that they name: `row_owner`: in the rows of one device no key range is named by more than 2048 rows, a bound that some block reaches.
All inputs are finite; a program needn't handle non-finite values.
Results may differ from the reference program's by a relative error of at most 0.0003.
Values sent between devices are 32-bit elements; how exact they have to be, the bound alone decides.
No kernel may reach another device: no remote copies, remote signals or barrier semaphores. Data moves between devices by JAX's collectives and lax.ppermute only.
A program may use at most 64 MiB of HBM per device.

```python
import math
import jax
import jax.numpy as jnp
import numpy as np

M = 256
KEYS = 4096
ROWS_DEV = 4096
ROWS = 131072
RANGE = 1024
CAP = 2048
N_DOM = 4


def draw_key_offset(key, part):
    order_key = jax.random.fold_in(key, 11)
    kept_key = jax.random.fold_in(key, 12)
    first_key = jax.random.fold_in(key, 13)
    second_key = jax.random.fold_in(key, 14)
    inner_offsets = (jax.random.permutation(order_key, RANGE - 2) + 1).astype(jnp.int32)
    end_offsets = jnp.array([0, RANGE - 1], jnp.int32)
    kept_offsets = jnp.concatenate([end_offsets, inner_offsets[4:]])
    kept_offsets = jax.random.permutation(kept_key, kept_offsets).astype(jnp.int32)
    first_draw = jax.random.randint(first_key, (ROWS,), 0, RANGE - 4, dtype=jnp.int32)
    second_draw = jax.random.randint(second_key, (ROWS,), 0, RANGE - 4, dtype=jnp.int32)
    return kept_offsets[jnp.minimum(first_draw, second_draw)].astype(jnp.int32)


def block_levels(rng, shape, shards, least, top_value):
    factor_of = 1.0
    for axis_at, parts in shards:
        steps = jax.random.uniform(jax.random.fold_in(jax.random.fold_in(rng, 6), axis_at), (parts,), jnp.float32, least / len(shards), top_value / len(shards))
        factor_of = factor_of * jnp.repeat(jnp.exp(steps), shape[axis_at] // parts).reshape((-1,) + (1,) * (len(shape) - 1 - axis_at))
    return factor_of


def shared_out(stream_key, own, number, rows, amount, top, reach, skew):
    order = jax.random.permutation(stream_key, amount)
    packed, usual = shares(amount, rows * top, reach, skew, True), shares(amount, rows * top, reach, skew, False)
    places = jnp.arange(amount)

    def named(tallies, rotation):
        used = int((tallies > 0).sum())
        fixed = max(1, used // 4)
        shifted = fixed + (places - fixed + rotation * (used - fixed)) % max(1, amount - fixed)
        return jnp.zeros((amount,), jnp.int32).at[order[jnp.where(places < fixed, places, shifted)]].set(jnp.asarray(tallies, jnp.int32))

    tallies = jnp.where(number % 4 == 0, named(packed, number // 4), named(usual, number - number // 4 - 1))
    mixed = jax.random.permutation(jax.random.fold_in(own, 3), amount)
    source_of, taker = mixed[0:amount // 2 * 2:2], mixed[1:amount // 2 * 2:2]
    slack = jnp.minimum(tallies[source_of] - 1, reach - tallies[taker]) // 2
    slack = jnp.where((source_of == order[0]) | (taker == order[0]) | (tallies[taker] == 0), 0, jnp.maximum(slack, 0))
    shifted = jax.random.randint(jax.random.fold_in(own, 4), (amount // 2,), 0, 1 << 20) % (slack + 1)
    tallies = tallies.at[source_of].add(-shifted).at[taker].add(shifted)
    items = jnp.searchsorted(jnp.cumsum(tallies), jnp.arange(rows * top), side="right").astype(jnp.int32)
    grid = items.reshape(top, rows).T
    grid = grid[jax.random.permutation(jax.random.fold_in(own, 1), rows)]
    rotation = jax.random.randint(jax.random.fold_in(own, 2), (rows, 1), 0, top)
    return jnp.take_along_axis(grid, (jnp.arange(top)[None, :] + rotation) % top, axis=1)


def shares(count, total, most, slope, full):
    portions = [(1 << 20) // math.isqrt(grade ** slope) + 1 for grade in range(1, count + 1)]
    largest = most if full else min(most, max(-(-total // count), total * portions[0] // sum(portions)))
    least = 1 if total - largest >= count - 1 else 0
    holding, rest = [largest] + [least] * (count - 1), total - largest - least * (count - 1)
    while rest > 0:
        free = [i for i in range(1, count) if holding[i] < largest] or [i for i in range(1, count) if holding[i] < most]
        mass, remaining = sum([portions[i] for i in free]), rest
        for i in free:
            more = min(most - holding[i], max(1, remaining * portions[i] // mass), rest)
            holding[i] = holding[i] + more
            rest = rest - more
    return np.array(holding)


def centred(own_key, extent, deviation, bound, split=(), held_as=jnp.bfloat16):
    result = deviation * jax.random.normal(own_key, extent, jnp.float32)
    if split:
        result = result * block_levels(own_key, extent, split, -0.22, 0.18)
    return jnp.clip(result, -bound, bound).astype(held_as)


def setup_inputs(seed: int = 0) -> dict:
    splits = jax.random.split(jax.random.key(seed), 4)
    facts = centred(splits[0], (ROWS, M), 1.0, 6.0, ((0, 32),), jnp.float32)
    row_owner_keys = jax.random.split(jax.random.fold_in(splits[1], 1), ROWS // ROWS_DEV)
    row_owner_turns = jax.random.permutation(jax.random.fold_in(splits[1], 3), ROWS // ROWS_DEV)
    row_owner = jax.vmap(lambda own, number: shared_out(jax.random.fold_in(splits[1], 2), own, number, ROWS_DEV, N_DOM, 1, CAP, 2))(row_owner_keys, row_owner_turns).reshape((ROWS, 1))
    key_offset = draw_key_offset(jax.random.fold_in(splits[3], 71), 0)
    return dict(facts=facts, row_owner=row_owner, key_offset=key_offset)


def reference(facts, row_owner, key_offset):
    key_ids = row_owner[:, 0] * (KEYS // N_DOM) + key_offset
    key_sums = jax.ops.segment_sum(facts, key_ids, num_segments=KEYS)
    key_counts = jax.ops.segment_sum(jnp.ones(key_ids.shape, jnp.float32), key_ids, num_segments=KEYS)
    key_means = key_sums / jnp.maximum(key_counts, 1.0)[:, None]
    return key_means, key_counts
```

```python
import functools

import jax
import jax.numpy as jnp
from jax import lax
from jax.experimental import pallas as pl
from jax.experimental.pallas import tpu as pltpu
from jax.sharding import PartitionSpec as P

KEYS = 4096
LANES = 128
SUB = 8
TABLES = 4
CHUNKS = 8
AXES = ("dom", "rep")


def bits_of(size):
    return [1 << b for b in range(size.bit_length() - 1)]


def local_kernel(me_ref, owner_ref, offset_ref, facts, *rest, outs, span, block, tiles):
    out_refs = rest[: len(outs)]
    tables = rest[len(outs) : len(outs) + TABLES]
    buf, addr_v, addr_s, sem, addr_sem = rest[len(outs) + TABLES :]
    rows = buf.shape[0]
    step = rows // CHUNKS
    copies = [
        pltpu.make_async_copy(
            facts.at[pl.ds(i * step, step)], buf.at[pl.ds(i * step, step)], sem.at[i]
        )
        for i in range(CHUNKS)
    ]
    for copy in copies:
        copy.start()
    key = (owner_ref[...] * span + offset_ref[...]) ^ (me_ref[0] * block)
    addr_v[...] = (key >> 3) * (SUB * tiles) + (key & (SUB - 1))
    addr_copy = pltpu.make_async_copy(addr_v, addr_s, addr_sem)
    addr_copy.start()

    n_blocks = KEYS // block
    groups = owner_ref.shape[0]

    def count(i, total):
        k = (owner_ref[pl.ds(i, 1), :] * span + offset_ref[pl.ds(i, 1), :]) ^ (me_ref[0] * block)
        high = (k // block == lax.broadcasted_iota(jnp.int32, (n_blocks, LANES), 0))
        low = (k % block == lax.broadcasted_iota(jnp.int32, (LANES, LANES), 0))
        return total + lax.dot_general(
            high.astype(jnp.float32).astype(jnp.bfloat16),
            low.astype(jnp.float32).astype(jnp.bfloat16),
            (((1,), (1,)), ((), ())),
            preferred_element_type=jnp.float32,
        )

    counts = lax.fori_loop(0, groups, count, jnp.zeros((n_blocks, LANES), jnp.float32))

    zero_rows = 8 * SUB

    def zero(i, _):
        for t in tables:
            t[pl.ds(pl.multiple_of(i * zero_rows, zero_rows), zero_rows), :] = jnp.zeros(
                (zero_rows, LANES), jnp.float32
            )
        return 0

    lax.fori_loop(0, KEYS * tiles // zero_rows, zero, 0)
    addr_copy.wait()
    per_group = SUB * tiles
    groups_step = step // per_group
    for c in range(CHUNKS):
        copies[c].wait()

        def add_rows(g, _):
            base = c * step + g * per_group
            first = (c * groups_step + g) * SUB
            for j in range(SUB):
                table = tables[j % TABLES]
                r = first + j
                at = pl.ds(addr_s[r // LANES, r % LANES], tiles, stride=SUB)
                table[at, :] = table[at, :] + buf[pl.ds(base + j, tiles, stride=SUB), :]
            return 0

        lax.fori_loop(0, groups_step, add_rows, 0, unroll=2)

    part = block * tiles
    for out, ids in zip(out_refs, outs):
        for at, b in enumerate(ids):
            size = min(part, 64)

            def total(i, _):
                d = pl.multiple_of(i * size, size)
                s = tables[0][pl.ds(b * part + d, size), :]
                for t in tables[1:]:
                    s = s + t[pl.ds(b * part + d, size), :]
                out[at, pl.ds(d, size), :] = s
                return 0

            lax.fori_loop(0, part // size, total, 0)
            out[at, pl.ds(part, SUB), :] = jnp.broadcast_to(counts[b : b + 1, :], (SUB, LANES))


def local_table(facts, owner, offset, me, outs, span, block):
    rows, width = facts.shape
    tiles = width // LANES
    view = facts.reshape(rows // SUB, SUB, tiles, LANES).transpose(0, 2, 1, 3)
    view = view.reshape(rows * tiles, LANES)
    lanes = (rows // LANES, LANES)
    vmem = pl.BlockSpec(memory_space=pltpu.VMEM)
    unit = block * tiles + SUB
    return pl.pallas_call(
        functools.partial(local_kernel, outs=outs, span=span, block=block, tiles=tiles),
        out_shape=[jax.ShapeDtypeStruct((len(ids), unit, LANES), jnp.float32) for ids in outs],
        in_specs=[
            pl.BlockSpec(memory_space=pltpu.SMEM),
            vmem,
            vmem,
            pl.BlockSpec(memory_space=pl.ANY),
        ],
        out_specs=[vmem] * len(outs),
        scratch_shapes=[pltpu.VMEM((KEYS * tiles, LANES), jnp.float32)] * TABLES
        + [
            pltpu.VMEM((rows * tiles, LANES), jnp.float32),
            pltpu.VMEM(lanes, jnp.int32),
            pltpu.SMEM(lanes, jnp.int32),
            pltpu.SemaphoreType.DMA((CHUNKS,)),
            pltpu.SemaphoreType.DMA,
        ],
        compiler_params=pltpu.CompilerParams(vmem_limit_bytes=32 << 20),
        name="local_table",
    )(me, owner.reshape(lanes), offset.reshape(lanes), view)


def route_kernel(*refs, n_in, outs):
    ins, out_refs = refs[:n_in], refs[n_in:]
    unit = ins[0].shape[1]
    for out, blocks in zip(out_refs, outs):
        for at, terms in enumerate(blocks):
            total = ins[terms[0][0]][terms[0][1]]
            for which, where in terms[1:]:
                total = total + ins[which][where]
            out[at] = total


def route(ins, outs):
    unit = ins[0].shape[1]
    vmem = pl.BlockSpec(memory_space=pltpu.VMEM)
    return pl.pallas_call(
        functools.partial(route_kernel, n_in=len(ins), outs=outs),
        out_shape=[jax.ShapeDtypeStruct((len(b), unit, LANES), jnp.float32) for b in outs],
        in_specs=[vmem] * len(ins),
        out_specs=[vmem] * len(outs),
        compiler_params=pltpu.CompilerParams(vmem_limit_bytes=16 << 20),
        name="route",
    )(*ins)


def finish_kernel(kept, arrived, means, counts, *, block, tiles):
    part = block * tiles
    row = kept[0, part : part + 1, :] + arrived[0, part : part + 1, :]
    counts[...] = row[:, :block]
    diagonal = lax.broadcasted_iota(jnp.int32, (block, LANES), 0) == lax.broadcasted_iota(
        jnp.int32, (block, LANES), 1
    )
    column = jnp.sum(jnp.where(diagonal, row, 0.0), axis=1, keepdims=True)
    column = jnp.maximum(column, 1.0)
    for g in range(block // SUB):
        for t in range(tiles):
            at = (g * tiles + t) * SUB
            total = kept[0, at : at + SUB, :] + arrived[0, at : at + SUB, :]
            means[g * SUB : (g + 1) * SUB, t * LANES : (t + 1) * LANES] = (
                total / column[g * SUB : (g + 1) * SUB, :]
            )


def finish(kept, arrived, block, tiles):
    vmem = pl.BlockSpec(memory_space=pltpu.VMEM)
    means, counts = pl.pallas_call(
        functools.partial(finish_kernel, block=block, tiles=tiles),
        out_shape=[
            jax.ShapeDtypeStruct((block, tiles * LANES), jnp.float32),
            jax.ShapeDtypeStruct((1, block), jnp.float32),
        ],
        in_specs=[vmem] * 2,
        out_specs=[vmem] * 2,
        compiler_params=pltpu.CompilerParams(vmem_limit_bytes=16 << 20),
        name="finish",
    )(kept, arrived)
    return means, counts.reshape(block)


def ordered(bits):
    ids = [0]
    for b in reversed(bits):
        ids = ids + [i | b for i in ids]
    return ids


def per_device(facts, row_owner, key_offset):
    n_dom, n_rep = lax.axis_size("dom"), lax.axis_size("rep")
    block = KEYS // (n_dom * n_rep)
    span = KEYS // n_dom
    tiles = facts.shape[1] // LANES
    me = (lax.axis_index("dom") * n_rep + lax.axis_index("rep")).astype(jnp.int32).reshape(1)
    devices = n_dom * n_rep

    def swap(x, bit):
        return lax.ppermute(x, AXES, [(i, i ^ bit) for i in range(devices)])

    bits = [n_rep * b for b in bits_of(n_dom)] + bits_of(n_rep)
    first, second, third, *middle, last = bits
    ids_a = ordered([second, third, *middle])
    ids_b = [i | last for i in ordered([third, second, *middle])]
    half = len(ids_a) // 2
    keep_ids = ids_a[half:] + ids_b[half:] + ids_a[:half] + ids_b[:half]
    send_ids = [i | first for i in keep_ids]
    sent, kept = local_table(
        facts, row_owner[:, 0], key_offset, me, (send_ids, keep_ids), span, block
    )
    got = swap(sent, first)

    def both(which):
        return [(0, which), (1, which)]

    send_a, send_b, keep = route(
        (kept, got),
        (
            [both(i) for i in range(half)],
            [both(half + i) for i in range(half)],
            [both(2 * half + i) for i in range(2 * half)],
        ),
    )
    got_a, got_b = swap(send_a, second), swap(send_b, third)
    quarter = half // 2
    send_a, send_b, keep = route(
        (keep, got_a, got_b),
        (
            [[(0, quarter + i), (1, quarter + i)] for i in range(quarter)],
            [[(0, half + quarter + i), (2, quarter + i)] for i in range(quarter)],
            [[(0, i), (1, i)] for i in range(quarter)]
            + [[(0, half + i), (2, i)] for i in range(quarter)],
        ),
    )
    got_a, got_b = swap(send_a, third), swap(send_b, second)
    pieces = [[(0, i), (1, i)] for i in range(quarter)] + [
        [(0, quarter + i), (2, i)] for i in range(quarter)
    ]
    ins = (keep, got_a, got_b)
    n = quarter
    for bit in middle:
        n = n // 2
        sent, keep = route(
            ins,
            (
                pieces[n : 2 * n] + pieces[3 * n : 4 * n],
                pieces[:n] + pieces[2 * n : 3 * n],
            ),
        )
        ins = (keep, swap(sent, bit))
        pieces = [both(i) for i in range(2 * n)]
    sent, keep = route(ins, (pieces[1:], pieces[:1]))
    return finish(keep, swap(sent, last), block, tiles)


def solution(mesh):
    placed = (P(AXES, None), P(AXES, None), P(AXES))
    return jax.shard_map(
        per_device,
        mesh=mesh,
        in_specs=placed,
        out_specs=(P(AXES, None), P(AXES)),
        check_vma=False,
    )
```

```python
import functools

import jax
import jax.numpy as jnp
from jax import lax
from jax.experimental import pallas as pl
from jax.experimental.pallas import tpu as pltpu
from jax.sharding import PartitionSpec as P

KEYS = 4096
LANES = 128
SUB = 8
TABLES = 4
AXES = ("dom", "rep")
VMEM = pl.BlockSpec(memory_space=pltpu.VMEM)


def bits_of(size):
    return [b for b in range(size.bit_length() - 1)]


class Plan:
    def __init__(self, n_dom, n_rep, rows, width):
        self.devices = n_dom * n_rep
        self.block = KEYS // self.devices
        self.span = KEYS // n_dom
        self.tiles = width // LANES
        self.rows = rows
        self.group = SUB * (self.tiles + 1)
        self.groups = self.block // SUB
        self.part = self.block * self.tiles
        self.unit = self.part + SUB
        rep = bits_of(n_rep)
        dom = [len(rep) + b for b in bits_of(n_dom)]
        self.core, self.second, self.third, *self.middle, self.last = dom + rep
        self.even = [self.core, self.last, self.second, self.third, *self.middle]
        self.odd = [self.core, self.last, self.third, self.second, *self.middle]
        self.chunk = self.devices // 4

    def virtual(self, place, order):
        out = jnp.zeros_like(place)
        for at, bit in enumerate(reversed(order)):
            out = out | (((place >> bit) & 1) << at)
        return out

    def pairs(self, even_bit, odd_bit):
        odd = 1 << self.core
        return [
            (i, i ^ (1 << (odd_bit if i & odd else even_bit))) for i in range(self.devices)
        ]


def sum_block(plan, tables, base, out, at, arrived):
    row = lax.broadcasted_iota(jnp.int32, (SUB, LANES), 0)
    lane = lax.broadcasted_iota(jnp.int32, (SUB, LANES), 1)
    first = pl.multiple_of(base * (plan.groups * plan.group), SUB)
    counts = jnp.zeros((SUB, LANES), jnp.float32)
    for g in range(plan.groups):
        for t in range(plan.tiles + 1):
            d = pl.ds(first + g * plan.group + t * SUB, SUB)
            total = tables[0][d, :]
            for table in tables[1:]:
                total = total + table[d, :]
            if t == plan.tiles:
                counts = jnp.where(lane == row + g * SUB, total, counts)
                continue
            to = pl.ds((g * plan.tiles + t) * SUB, SUB)
            for ref, where in arrived:
                total = total + ref[where, to, :]
            out[at, to, :] = total
    to = pl.ds(plan.part, SUB)
    total = jnp.broadcast_to(jnp.sum(counts, axis=0, keepdims=True), (SUB, LANES))
    for ref, where in arrived:
        total = total + ref[where, to, :]
    out[at, to, :] = total


def table_kernel(plan, me_ref, owner, offset, facts, sent, *rest):
    tables = rest[:TABLES]
    buf, owner_v, offset_v, addr_v, addr_s, same_v, same_s, sem, small = rest[TABLES:]
    n = plan.rows // LANES
    half = n // 2
    per = LANES // SUB
    wide = plan.tiles * SUB

    def fetch(i):
        d = pl.ds(i * per, per)
        return pltpu.make_async_copy(facts.at[d], buf.at[d, pl.ds(0, wide)], sem.at[i])

    copies = [
        pltpu.make_async_copy(owner, owner_v, small.at[0]),
        pltpu.make_async_copy(offset, offset_v, small.at[1]),
    ]
    for copy in copies:
        copy.start()
    for i in range(half):
        fetch(i).start()
        fetch(half + i).start()

    def zero(refs):
        step = SUB * SUB

        def body(i, _):
            for t in refs:
                t[pl.ds(pl.multiple_of(i * step, step), step), :] = jnp.zeros(
                    (step, LANES), jnp.float32
                )
            return 0

        lax.fori_loop(0, refs[0].shape[0] // step, body, 0)

    zero(tables[: TABLES // 2])
    for copy in copies:
        copy.wait()
    me = me_ref[0]
    key = owner_v[...] * plan.span + offset_v[...]
    shift = plan.block.bit_length() - 1
    owner_core = (key >> (shift + plan.core)) & 1
    place = (key >> shift) ^ me
    place = jnp.where(
        owner_core == 1, plan.virtual(place, plan.odd), plan.virtual(place, plan.even)
    )
    key = (place << shift) | (key & (plan.block - 1))
    addr = (key >> 3) * plan.group + (key & (SUB - 1))
    addr_v[...] = addr
    same_v[...] = jnp.where(addr[:half] == addr[half:], 1.0, 0.0)
    copies = [
        pltpu.make_async_copy(addr_v, addr_s, small.at[2]),
        pltpu.make_async_copy(same_v, same_s, small.at[3]),
    ]
    for copy in copies:
        copy.start()
    zero(tables[TABLES // 2 :])

    def ones(i, _):
        for j in range(per):
            buf[i * per + j, pl.ds(wide, SUB), :] = jnp.ones((SUB, LANES), jnp.float32)
        return 0

    lax.fori_loop(0, n, ones, 0)
    for copy in copies:
        copy.wait()

    def add_rows(i, _):
        fetch(i).wait()
        fetch(half + i).wait()
        for j in range(LANES):
            table = tables[j % TABLES]
            one = pl.ds(addr_s[i, j], plan.tiles + 1, stride=SUB)
            two = pl.ds(addr_s[half + i, j], plan.tiles + 1, stride=SUB)
            lines = pl.ds(j % SUB, plan.tiles + 1, stride=SUB)
            row_one = buf[i * per + j // SUB, lines, :]
            row_two = buf[(half + i) * per + j // SUB, lines, :]
            old_one = table[one, :]
            old_two = table[two, :]
            table[one, :] = old_one + row_one
            table[two, :] = old_two + (row_two + same_s[i, j] * row_one)
        return 0

    lax.fori_loop(0, half, add_rows, 0)

    def send(i, _):
        sum_block(plan, tables, 3 * plan.chunk + i, sent, i, ())
        return 0

    lax.fori_loop(0, plan.chunk, send, 0)


def make_table(plan, me, owner, offset, facts):
    rows = plan.rows
    view = facts.reshape(rows // SUB, SUB, plan.tiles, LANES).transpose(0, 2, 1, 3)
    view = view.reshape(rows // SUB, plan.tiles * SUB, LANES)
    lanes = (rows // LANES, LANES)
    half = (rows // LANES // 2, LANES)
    far = [
        pltpu.with_memory_space_constraint(x, pltpu.HBM)
        for x in (owner.reshape(lanes), offset.reshape(lanes), view)
    ]
    hbm = pl.BlockSpec(memory_space=pltpu.HBM)
    table = jax.ShapeDtypeStruct((KEYS // SUB * plan.group, LANES), jnp.float32)
    return pl.pallas_call(
        functools.partial(table_kernel, plan),
        out_shape=[jax.ShapeDtypeStruct((plan.chunk, plan.unit, LANES), jnp.float32)]
        + [table] * TABLES,
        in_specs=[pl.BlockSpec(memory_space=pltpu.SMEM), hbm, hbm, hbm],
        out_specs=[VMEM] * (1 + TABLES),
        scratch_shapes=[
            pltpu.VMEM((rows // SUB, plan.group, LANES), jnp.float32),
            pltpu.VMEM(lanes, jnp.int32),
            pltpu.VMEM(lanes, jnp.int32),
            pltpu.VMEM(lanes, jnp.int32),
            pltpu.SMEM(lanes, jnp.int32),
            pltpu.VMEM(half, jnp.float32),
            pltpu.SMEM(half, jnp.float32),
            pltpu.SemaphoreType.DMA((rows // LANES,)),
            pltpu.SemaphoreType.DMA((4,)),
        ],
        compiler_params=pltpu.CompilerParams(vmem_limit_bytes=12 << 20),
        name="make_table",
    )(me, *far)


def send_kernel(plan, base, first, n_got, *refs):
    tables, got, out = refs[:TABLES], refs[TABLES : TABLES + n_got], refs[-1]

    def body(i, _):
        sum_block(plan, tables, base + first + i, out, i, [(g, first + i) for g in got])
        return 0

    lax.fori_loop(0, out.shape[0], body, 0)


def send_blocks(plan, tables, got, base, first, count):
    n = len(tables) + len(got)
    return pl.pallas_call(
        functools.partial(send_kernel, plan, base, first, len(got)),
        out_shape=jax.ShapeDtypeStruct((count, plan.unit, LANES), jnp.float32),
        in_specs=[VMEM] * n,
        out_specs=VMEM,
        compiler_params=pltpu.CompilerParams(vmem_limit_bytes=4 << 20),
        name="send_blocks",
    )(*tables, *got)


def finish_kernel(plan, n_got, *refs):
    tables, got = refs[:TABLES], refs[TABLES : TABLES + n_got]
    means, counts, total = refs[TABLES + n_got :]
    sum_block(plan, tables, 0, total, 0, [(g, 0) for g in got])
    row = total[0, pl.ds(plan.part, 1), :]
    counts[...] = row[:, : plan.block]
    shape = (plan.block, LANES)
    diagonal = lax.broadcasted_iota(jnp.int32, shape, 0) == lax.broadcasted_iota(
        jnp.int32, shape, 1
    )
    column = jnp.sum(jnp.where(diagonal, row, 0.0), axis=1, keepdims=True)
    column = jnp.maximum(column, 1.0)
    for g in range(plan.groups):
        for t in range(plan.tiles):
            means[g * SUB : (g + 1) * SUB, t * LANES : (t + 1) * LANES] = (
                total[0, pl.ds((g * plan.tiles + t) * SUB, SUB), :]
                / column[g * SUB : (g + 1) * SUB, :]
            )


def finish(plan, tables, got):
    means, counts = pl.pallas_call(
        functools.partial(finish_kernel, plan, len(got)),
        out_shape=[
            jax.ShapeDtypeStruct((plan.block, plan.tiles * LANES), jnp.float32),
            jax.ShapeDtypeStruct((1, plan.block), jnp.float32),
        ],
        in_specs=[VMEM] * (len(tables) + len(got)),
        out_specs=[VMEM] * 2,
        scratch_shapes=[pltpu.VMEM((1, plan.unit, LANES), jnp.float32)],
        compiler_params=pltpu.CompilerParams(vmem_limit_bytes=4 << 20),
        name="finish",
    )(*tables, *got)
    return means, counts.reshape(plan.block)


def per_device(facts, row_owner, key_offset):
    n_dom, n_rep = lax.axis_size("dom"), lax.axis_size("rep")
    plan = Plan(n_dom, n_rep, *facts.shape)
    me = (lax.axis_index("dom") * n_rep + lax.axis_index("rep")).astype(jnp.int32).reshape(1)

    def swap(x, even_bit, odd_bit=None):
        odd_bit = even_bit if odd_bit is None else odd_bit
        return lax.ppermute(x, AXES, plan.pairs(even_bit, odd_bit))

    sent, *tables = make_table(plan, me, row_owner[:, 0], key_offset, facts)
    chunk = plan.chunk
    got_q = [swap(sent, plan.core)]
    got_p = [swap(send_blocks(plan, tables, [], 2 * chunk, 0, chunk), plan.core)]
    stages = [(plan.second, plan.third), (plan.third, plan.second)]
    stages += [(bit, bit) for bit in plan.middle]
    size = chunk
    for stage in stages:
        size //= 2
        for got, base in ((got_q, chunk), (got_p, 0)):
            got.append(swap(send_blocks(plan, tables, got, base, size, size), *stage))
    got_p.append(swap(send_blocks(plan, tables, got_q, chunk, 0, 1), plan.last))
    return finish(plan, tables, got_p)


def solution(mesh):
    placed = (P(AXES, None), P(AXES, None), P(AXES))
    return jax.shard_map(
        per_device,
        mesh=mesh,
        in_specs=placed,
        out_specs=(P(AXES, None), P(AXES)),
        check_vma=False,
    )
```

```python
import functools

import jax
import jax.numpy as jnp
from jax import lax
from jax.experimental import pallas as pl
from jax.experimental.pallas import tpu as pltpu
from jax.sharding import PartitionSpec as P

KEYS = 4096
LANES = 128
SUB = 8
TABLES = 4
AXES = ("dom", "rep")
VMEM = pl.BlockSpec(memory_space=pltpu.VMEM)


def bits_of(size):
    return [b for b in range(size.bit_length() - 1)]


class Plan:
    def __init__(self, n_dom, n_rep, rows, width):
        self.devices = n_dom * n_rep
        self.block = KEYS // self.devices
        self.span = KEYS // n_dom
        self.tiles = width // LANES
        self.rows = rows
        self.group = SUB * (self.tiles + 1)
        self.groups = self.block // SUB
        self.part = self.block * self.tiles
        self.unit = self.part + SUB
        rep = bits_of(n_rep)
        dom = [len(rep) + b for b in bits_of(n_dom)]
        self.core, self.second, self.third, self.near, *self.middle, self.far = dom + rep
        head = [self.core, self.far, self.near]
        self.even = [*head, self.second, self.third, *self.middle]
        self.odd = [*head, self.third, self.second, *self.middle]
        self.chunk = self.devices // 8

    def virtual(self, place, order):
        out = jnp.zeros_like(place)
        for at, bit in enumerate(reversed(order)):
            out = out | (((place >> bit) & 1) << at)
        return out

    def pairs(self, even_bit, odd_bit):
        odd = 1 << self.core
        return [
            (i, i ^ (1 << (odd_bit if i & odd else even_bit))) for i in range(self.devices)
        ]


def sum_block(plan, tables, base, out, at, arrived):
    row = lax.broadcasted_iota(jnp.int32, (SUB, LANES), 0)
    lane = lax.broadcasted_iota(jnp.int32, (SUB, LANES), 1)
    first = pl.multiple_of(base * (plan.groups * plan.group), SUB)
    counts = jnp.zeros((SUB, LANES), jnp.float32)
    for g in range(plan.groups):
        for t in range(plan.tiles + 1):
            d = pl.ds(first + g * plan.group + t * SUB, SUB)
            total = tables[0][d, :]
            for table in tables[1:]:
                total = total + table[d, :]
            if t == plan.tiles:
                counts = jnp.where(lane == row + g * SUB, total, counts)
                continue
            to = pl.ds((g * plan.tiles + t) * SUB, SUB)
            for ref, where in arrived:
                total = total + ref[where, to, :]
            out[at, to, :] = total
    to = pl.ds(plan.part, SUB)
    total = jnp.broadcast_to(jnp.sum(counts, axis=0, keepdims=True), (SUB, LANES))
    for ref, where in arrived:
        total = total + ref[where, to, :]
    out[at, to, :] = total


def table_kernel(plan, n_rep, owner, offset, facts, sent, *rest):
    tables = rest[:TABLES]
    buf, owner_v, offset_v, addr_v, addr_s, same_v, same_s, sem, small = rest[TABLES:]
    n = plan.rows // LANES
    half = n // 2
    per = LANES // SUB
    wide = plan.tiles * SUB

    def fetch(i):
        d = pl.ds(i * per, per)
        return pltpu.make_async_copy(facts.at[d], buf.at[d, pl.ds(0, wide)], sem.at[i])

    copies = [
        pltpu.make_async_copy(owner, owner_v, small.at[0]),
        pltpu.make_async_copy(offset, offset_v, small.at[1]),
    ]
    for copy in copies:
        copy.start()
    for i in range(half):
        fetch(i).start()
        fetch(half + i).start()

    def zero(refs):
        step = SUB * SUB

        def body(i, _):
            for t in refs:
                t[pl.ds(pl.multiple_of(i * step, step), step), :] = jnp.zeros(
                    (step, LANES), jnp.float32
                )
            return 0

        lax.fori_loop(0, refs[0].shape[0] // step, body, 0)

    zero(tables[: TABLES // 2])
    for copy in copies:
        copy.wait()
    me = lax.axis_index(AXES[0]) * n_rep + lax.axis_index(AXES[1])
    key = owner_v[...] * plan.span + offset_v[...]
    shift = plan.block.bit_length() - 1
    owner_core = (key >> (shift + plan.core)) & 1
    place = (key >> shift) ^ me
    place = jnp.where(
        owner_core == 1, plan.virtual(place, plan.odd), plan.virtual(place, plan.even)
    )
    key = (place << shift) | (key & (plan.block - 1))
    addr = (key >> 3) * plan.group + (key & (SUB - 1))
    addr_v[...] = addr
    same_v[...] = jnp.where(addr[:half] == addr[half:], 1.0, 0.0)
    copies = [
        pltpu.make_async_copy(addr_v, addr_s, small.at[2]),
        pltpu.make_async_copy(same_v, same_s, small.at[3]),
    ]
    for copy in copies:
        copy.start()
    zero(tables[TABLES // 2 :])

    def ones(i, _):
        for j in range(per):
            buf[i * per + j, pl.ds(wide, SUB), :] = jnp.ones((SUB, LANES), jnp.float32)
        return 0

    lax.fori_loop(0, n, ones, 0)
    for copy in copies:
        copy.wait()

    def add_rows(i, _):
        fetch(i).wait()
        fetch(half + i).wait()
        for j in range(LANES):
            table = tables[j % TABLES]
            one = pl.ds(addr_s[i, j], plan.tiles + 1, stride=SUB)
            two = pl.ds(addr_s[half + i, j], plan.tiles + 1, stride=SUB)
            lines = pl.ds(j % SUB, plan.tiles + 1, stride=SUB)
            row_one = buf[i * per + j // SUB, lines, :]
            row_two = buf[(half + i) * per + j // SUB, lines, :]
            old_one = table[one, :]
            old_two = table[two, :]
            table[one, :] = old_one + row_one
            table[two, :] = old_two + (row_two + same_s[i, j] * row_one)
        return 0

    lax.fori_loop(0, half, add_rows, 0)

    def send(i, _):
        sum_block(plan, tables, 7 * plan.chunk + i, sent, i, ())
        return 0

    lax.fori_loop(0, plan.chunk, send, 0)


def make_table(plan, n_rep, owner, offset, facts):
    rows = plan.rows
    view = facts.reshape(rows // SUB, SUB, plan.tiles, LANES).transpose(0, 2, 1, 3)
    view = view.reshape(rows // SUB, plan.tiles * SUB, LANES)
    lanes = (rows // LANES, LANES)
    half = (rows // LANES // 2, LANES)
    far = [
        pltpu.with_memory_space_constraint(x, pltpu.HBM)
        for x in (owner.reshape(lanes), offset.reshape(lanes), view)
    ]
    hbm = pl.BlockSpec(memory_space=pltpu.HBM)
    table = jax.ShapeDtypeStruct((KEYS // SUB * plan.group, LANES), jnp.float32)
    return pl.pallas_call(
        functools.partial(table_kernel, plan, n_rep),
        out_shape=[jax.ShapeDtypeStruct((plan.chunk, plan.unit, LANES), jnp.float32)]
        + [table] * TABLES,
        in_specs=[hbm, hbm, hbm],
        out_specs=[VMEM] * (1 + TABLES),
        scratch_shapes=[
            pltpu.VMEM((rows // SUB, plan.group, LANES), jnp.float32),
            pltpu.VMEM(lanes, jnp.int32),
            pltpu.VMEM(lanes, jnp.int32),
            pltpu.VMEM(lanes, jnp.int32),
            pltpu.SMEM(lanes, jnp.int32),
            pltpu.VMEM(half, jnp.float32),
            pltpu.SMEM(half, jnp.float32),
            pltpu.SemaphoreType.DMA((rows // LANES,)),
            pltpu.SemaphoreType.DMA((4,)),
        ],
        compiler_params=pltpu.CompilerParams(vmem_limit_bytes=12 << 20),
        name="make_table",
    )(*far)


def send_kernel(plan, base, first, n_got, *refs):
    tables, got, out = refs[:TABLES], refs[TABLES : TABLES + n_got], refs[-1]

    def body(i, _):
        sum_block(plan, tables, base + first + i, out, i, [(g, first + i) for g in got])
        return 0

    lax.fori_loop(0, out.shape[0], body, 0)


def send_blocks(plan, tables, got, base, first, count):
    n = len(tables) + len(got)
    return pl.pallas_call(
        functools.partial(send_kernel, plan, base, first, len(got)),
        out_shape=jax.ShapeDtypeStruct((count, plan.unit, LANES), jnp.float32),
        in_specs=[VMEM] * n,
        out_specs=VMEM,
        compiler_params=pltpu.CompilerParams(vmem_limit_bytes=4 << 20),
        name="send_blocks",
    )(*tables, *got)


def finish_kernel(plan, n_got, *refs):
    tables, got = refs[:TABLES], refs[TABLES : TABLES + n_got]
    means, counts, total = refs[TABLES + n_got :]
    sum_block(plan, tables, 0, total, 0, [(g, 0) for g in got])
    row = total[0, pl.ds(plan.part, 1), :]
    counts[...] = row[:, : plan.block]
    shape = (plan.block, LANES)
    diagonal = lax.broadcasted_iota(jnp.int32, shape, 0) == lax.broadcasted_iota(
        jnp.int32, shape, 1
    )
    column = jnp.sum(jnp.where(diagonal, row, 0.0), axis=1, keepdims=True)
    column = jnp.maximum(column, 1.0)
    for g in range(plan.groups):
        for t in range(plan.tiles):
            means[g * SUB : (g + 1) * SUB, t * LANES : (t + 1) * LANES] = (
                total[0, pl.ds((g * plan.tiles + t) * SUB, SUB), :]
                / column[g * SUB : (g + 1) * SUB, :]
            )


def finish(plan, tables, got):
    means, counts = pl.pallas_call(
        functools.partial(finish_kernel, plan, len(got)),
        out_shape=[
            jax.ShapeDtypeStruct((plan.block, plan.tiles * LANES), jnp.float32),
            jax.ShapeDtypeStruct((1, plan.block), jnp.float32),
        ],
        in_specs=[VMEM] * (len(tables) + len(got)),
        out_specs=[VMEM] * 2,
        scratch_shapes=[pltpu.VMEM((1, plan.unit, LANES), jnp.float32)],
        compiler_params=pltpu.CompilerParams(vmem_limit_bytes=4 << 20),
        name="finish",
    )(*tables, *got)
    return means, counts.reshape(plan.block)


def per_device(facts, row_owner, key_offset):
    n_dom, n_rep = lax.axis_size("dom"), lax.axis_size("rep")
    plan = Plan(n_dom, n_rep, *facts.shape)

    def swap(x, even_bit, odd_bit=None):
        odd_bit = even_bit if odd_bit is None else odd_bit
        return lax.ppermute(x, AXES, plan.pairs(even_bit, odd_bit))

    sent, *tables = make_table(plan, n_rep, row_owner[:, 0], key_offset, facts)
    size = plan.chunk
    got = [[] for _ in range(4)]
    for c in reversed(range(4)):
        if c < 3:
            sent = send_blocks(plan, tables, [], (4 + c) * size, 0, size)
        got[c].append(swap(sent, plan.core))
    stages = [(plan.second, plan.third), (plan.third, plan.second)]
    stages += [(bit, bit) for bit in plan.middle]
    for stage in stages:
        size //= 2
        for c in reversed(range(4)):
            sent = send_blocks(plan, tables, got[c], c * plan.chunk, size, size)
            got[c].append(swap(sent, *stage))
    for c, to, bit in ((3, 2, plan.near), (1, 0, plan.near), (2, 0, plan.far)):
        sent = send_blocks(plan, tables, got[c], c * plan.chunk, 0, 1)
        got[to].append(swap(sent, bit))
    return finish(plan, tables, got[0])


def solution(mesh):
    placed = (P(AXES, None), P(AXES, None), P(AXES))
    return jax.shard_map(
        per_device,
        mesh=mesh,
        in_specs=placed,
        out_specs=(P(AXES, None), P(AXES)),
        check_vma=False,
    )
```

```python
import functools

import jax
import jax.numpy as jnp
from jax import lax
from jax.experimental import pallas as pl
from jax.experimental.pallas import tpu as pltpu
from jax.sharding import PartitionSpec as P


KEYS = 4096
LANES = 128
SUB = 8
TABLES = 4
AXES = ("dom", "rep")
VMEM = pl.BlockSpec(memory_space=pltpu.VMEM)


def bits_of(size):
    return [b for b in range(size.bit_length() - 1)]


class Plan:
    def __init__(self, n_dom, n_rep, rows, width):
        self.devices = n_dom * n_rep
        self.block = KEYS // self.devices
        self.span = KEYS // n_dom
        self.tiles = width // LANES
        self.rows = rows
        self.group = SUB * (self.tiles + 1)
        self.groups = self.block // SUB
        self.part = self.block * self.tiles
        self.unit = self.part + SUB
        self.all = tuple(range(self.tiles))
        rep = bits_of(n_rep)
        dom = [len(rep) + b for b in bits_of(n_dom)]
        self.core, self.second, self.third, self.near, *self.middle, self.far = dom + rep
        head = [self.core, self.far, self.near]
        self.even = [*head, self.second, self.third, *self.middle]
        self.odd = [*head, self.third, self.second, *self.middle]

    def blocks(self, **fixed):
        names = ["core", "far", "near", "first", "then"]
        names += [f"middle{i}" for i in range(len(self.middle))]
        weight = {n: 1 << at for at, n in enumerate(reversed(names))}
        return [
            b
            for b in range(self.devices)
            if all(bool(b & weight[n]) == bool(v) for n, v in fixed.items())
        ], weight

    def payload(self, blocks, cols, counted):
        lines = self.block * len(cols) + (SUB if counted else 0)
        return jax.ShapeDtypeStruct((len(blocks), lines, LANES), jnp.float32)

    def virtual(self, place, order):
        out = jnp.zeros_like(place)
        for at, bit in enumerate(reversed(order)):
            out = out | (((place >> bit) & 1) << at)
        return out

    def pairs(self, even_bit, odd_bit):
        odd = 1 << self.core
        return [
            (i, i ^ (1 << (odd_bit if i & odd else even_bit))) for i in range(self.devices)
        ]


def sum_block(plan, tables, base, out, at, arrived, cols, counted):
    first = pl.multiple_of(base * (plan.groups * plan.group), SUB)

    def table_sum(g, t):
        d = pl.ds(first + g * plan.group + t * SUB, SUB)
        total = tables[0][d, :]
        for table in tables[1:]:
            total = total + table[d, :]
        return total

    for g in range(plan.groups):
        for t in cols:
            total = table_sum(g, t)
            for ref, where, own in arrived:
                if t in own:
                    line = (g * len(own) + own.index(t)) * SUB
                    total = total + ref[where, pl.ds(line, SUB), :]
            line = (g * len(cols) + cols.index(t)) * SUB
            out[at, pl.ds(line, SUB), :] = total
    if counted:
        row = lax.broadcasted_iota(jnp.int32, (SUB, LANES), 0)
        lane = lax.broadcasted_iota(jnp.int32, (SUB, LANES), 1)
        counts = jnp.zeros((SUB, LANES), jnp.float32)
        for g in range(plan.groups):
            counts = jnp.where(lane == row + g * SUB, table_sum(g, plan.tiles), counts)
        total = jnp.broadcast_to(jnp.sum(counts, axis=0, keepdims=True), (SUB, LANES))
        for ref, where, own in arrived:
            line = plan.block * len(own)
            if ref.shape[1] > line:
                total = total + ref[where, pl.ds(line, SUB), :]
        out[at, pl.ds(plan.block * len(cols), SUB), :] = total


def table_kernel(plan, n_rep, entries, cols, counted, owner, offset, facts, sent, *rest):
    tables = rest[:TABLES]
    buf, owner_v, offset_v, addr_v, addr_s, same_v, same_s, sem, small = rest[TABLES:]
    n = plan.rows // LANES
    half = n // 2
    per = LANES // SUB
    wide = plan.tiles * SUB

    def fetch(i):
        d = pl.ds(i * per, per)
        return pltpu.make_async_copy(facts.at[d], buf.at[d, pl.ds(0, wide)], sem.at[i])

    copies = [
        pltpu.make_async_copy(owner, owner_v, small.at[0]),
        pltpu.make_async_copy(offset, offset_v, small.at[1]),
    ]
    for copy in copies:
        copy.start()
    for i in range(half):
        fetch(i).start()
        fetch(half + i).start()

    def zero(refs):
        step = SUB * SUB

        def body(i, _):
            for t in refs:
                t[pl.ds(pl.multiple_of(i * step, step), step), :] = jnp.zeros(
                    (step, LANES), jnp.float32
                )
            return 0

        lax.fori_loop(0, refs[0].shape[0] // step, body, 0)

    zero(tables[: TABLES // 2])
    for copy in copies:
        copy.wait()
    me = lax.axis_index(AXES[0]) * n_rep + lax.axis_index(AXES[1])
    key = owner_v[...] * plan.span + offset_v[...]
    shift = plan.block.bit_length() - 1
    owner_core = (key >> (shift + plan.core)) & 1
    place = (key >> shift) ^ me
    place = jnp.where(
        owner_core == 1, plan.virtual(place, plan.odd), plan.virtual(place, plan.even)
    )
    key = (place << shift) | (key & (plan.block - 1))
    addr = (key >> 3) * plan.group + (key & (SUB - 1))
    addr_v[...] = addr
    same_v[...] = jnp.where(addr[:half] == addr[half:], 1.0, 0.0)
    copies = [
        pltpu.make_async_copy(addr_v, addr_s, small.at[2]),
        pltpu.make_async_copy(same_v, same_s, small.at[3]),
    ]
    for copy in copies:
        copy.start()
    zero(tables[TABLES // 2 :])

    def ones(i, _):
        for j in range(per):
            buf[i * per + j, pl.ds(wide, SUB), :] = jnp.ones((SUB, LANES), jnp.float32)
        return 0

    lax.fori_loop(0, n, ones, 0)
    for copy in copies:
        copy.wait()

    def add_rows(i, _):
        fetch(i).wait()
        fetch(half + i).wait()
        for j in range(LANES):
            table = tables[j % TABLES]
            one = pl.ds(addr_s[i, j], plan.tiles + 1, stride=SUB)
            two = pl.ds(addr_s[half + i, j], plan.tiles + 1, stride=SUB)
            lines = pl.ds(j % SUB, plan.tiles + 1, stride=SUB)
            row_one = buf[i * per + j // SUB, lines, :]
            row_two = buf[(half + i) * per + j // SUB, lines, :]
            old_one = table[one, :]
            old_two = table[two, :]
            table[one, :] = old_one + row_one
            table[two, :] = old_two + (row_two + same_s[i, j] * row_one)
        return 0

    lax.fori_loop(0, half, add_rows, 0)

    send_runs(plan, tables, (), sent, entries, cols, counted)


def make_table(plan, n_rep, owner, offset, facts, blocks, cols, counted):
    rows = plan.rows
    view = facts.reshape(rows // SUB, SUB, plan.tiles, LANES).transpose(0, 2, 1, 3)
    view = view.reshape(rows // SUB, plan.tiles * SUB, LANES)
    lanes = (rows // LANES, LANES)
    half = (rows // LANES // 2, LANES)
    far = [
        pltpu.with_memory_space_constraint(x, pltpu.HBM)
        for x in (owner.reshape(lanes), offset.reshape(lanes), view)
    ]
    hbm = pl.BlockSpec(memory_space=pltpu.HBM)
    table = jax.ShapeDtypeStruct((KEYS // SUB * plan.group, LANES), jnp.float32)
    return pl.pallas_call(
        functools.partial(
            table_kernel, plan, n_rep, [(b, ()) for b in blocks], cols, counted
        ),
        out_shape=[plan.payload(blocks, cols, counted)]
        + [table] * TABLES,
        in_specs=[hbm, hbm, hbm],
        out_specs=[VMEM] * (1 + TABLES),
        scratch_shapes=[
            pltpu.VMEM((rows // SUB, plan.group, LANES), jnp.float32),
            pltpu.VMEM(lanes, jnp.int32),
            pltpu.VMEM(lanes, jnp.int32),
            pltpu.VMEM(lanes, jnp.int32),
            pltpu.SMEM(lanes, jnp.int32),
            pltpu.VMEM(half, jnp.float32),
            pltpu.SMEM(half, jnp.float32),
            pltpu.SemaphoreType.DMA((rows // LANES,)),
            pltpu.SemaphoreType.DMA((4,)),
        ],
        compiler_params=pltpu.CompilerParams(vmem_limit_bytes=12 << 20),
        name="make_table",
    )(*far)


def send_runs(plan, tables, arrays, out, entries, cols, counted):
    def follows(a, b):
        return b[0] == a[0] + 1 and [(k, u + 1, o) for k, u, o in a[1]] == list(b[1])

    start = 0
    while start < len(entries):
        end = start + 1
        while end < len(entries) and follows(entries[end - 1], entries[end]):
            end += 1
        block, terms = entries[start]

        def body(i, _):
            arrived = [(arrays[k], u + i, own) for k, u, own in terms]
            sum_block(plan, tables, block + i, out, start + i, arrived, cols, counted)
            return 0

        lax.fori_loop(0, end - start, body, 0)
        start = end


def send_kernel(plan, n_got, entries, cols, counted, *refs):
    tables, got, out = refs[:TABLES], refs[TABLES : TABLES + n_got], refs[-1]
    send_runs(plan, tables, got, out, entries, cols, counted)


def send_blocks(plan, tables, got, entries, cols, counted):
    n = len(tables) + len(got)
    return pl.pallas_call(
        functools.partial(send_kernel, plan, len(got), entries, cols, counted),
        out_shape=plan.payload(entries, cols, counted),
        in_specs=[VMEM] * n,
        out_specs=VMEM,
        compiler_params=pltpu.CompilerParams(vmem_limit_bytes=4 << 20),
        name="send_blocks",
    )(*tables, *got)


def finish_kernel(plan, n_got, terms, *refs):
    tables, got = refs[:TABLES], refs[TABLES : TABLES + n_got]
    means, counts, total = refs[TABLES + n_got :]
    arrived = [(got[k], u, own) for k, u, own in terms]
    sum_block(plan, tables, 0, total, 0, arrived, plan.all, True)
    row = total[0, pl.ds(plan.part, 1), :]
    counts[...] = row[:, : plan.block]
    shape = (plan.block, LANES)
    diagonal = lax.broadcasted_iota(jnp.int32, shape, 0) == lax.broadcasted_iota(
        jnp.int32, shape, 1
    )
    column = jnp.sum(jnp.where(diagonal, row, 0.0), axis=1, keepdims=True)
    column = jnp.maximum(column, 1.0)
    for g in range(plan.groups):
        for t in range(plan.tiles):
            means[g * SUB : (g + 1) * SUB, t * LANES : (t + 1) * LANES] = (
                total[0, pl.ds((g * plan.tiles + t) * SUB, SUB), :]
                / column[g * SUB : (g + 1) * SUB, :]
            )


def finish(plan, tables, got, terms):
    means, counts = pl.pallas_call(
        functools.partial(finish_kernel, plan, len(got), terms),
        out_shape=[
            jax.ShapeDtypeStruct((plan.block, plan.tiles * LANES), jnp.float32),
            jax.ShapeDtypeStruct((1, plan.block), jnp.float32),
        ],
        in_specs=[VMEM] * (len(tables) + len(got)),
        out_specs=[VMEM] * 2,
        scratch_shapes=[pltpu.VMEM((1, plan.unit, LANES), jnp.float32)],
        compiler_params=pltpu.CompilerParams(vmem_limit_bytes=4 << 20),
        name="finish",
    )(*tables, *got)
    return means, counts.reshape(plan.block)


def per_device(facts, row_owner, key_offset):
    n_dom, n_rep = lax.axis_size("dom"), lax.axis_size("rep")
    plan = Plan(n_dom, n_rep, *facts.shape)
    pairs = {
        "core": (plan.core, plan.core),
        "first": (plan.second, plan.third),
        "then": (plan.third, plan.second),
        "near": (plan.near, plan.near),
        "far": (plan.far, plan.far),
    }
    extra = middle_names(len(plan.middle))
    pairs |= {n: (bit, bit) for n, bit in zip(extra, plan.middle)}
    middle = len(plan.all) // 2
    left, right = plan.all[:middle], plan.all[middle:]
    arrived = {}
    tables = None

    def entries_of(blocks, cols):
        got, entries = [], []
        for b in blocks:
            terms = []
            for array, unit, own in arrived.get(b, []):
                if not set(own) & set(cols):
                    continue
                at = [i for i, g in enumerate(got) if g is array]
                if not at:
                    at = [len(got)]
                    got.append(array)
                terms.append((at[0], unit, own))
            entries.append((b, tuple(terms)))
        return got, entries

    parts = {"left": (left, True), "right": (right, False), "whole": (plan.all, True)}
    for bit, which, fixed in schedule(extra):
        cols, counted = parts[which]
        blocks, weight = plan.blocks(**{bit: 1}, **fixed)
        if tables is None:
            sent, *tables = make_table(
                plan, n_rep, row_owner[:, 0], key_offset, facts, blocks, cols, counted
            )
        else:
            got, entries = entries_of(blocks, cols)
            sent = send_blocks(plan, tables, got, entries, cols, counted)
        array = lax.ppermute(sent, AXES, plan.pairs(*pairs[bit]))
        for unit, b in enumerate(blocks):
            arrived.setdefault(b - weight[bit], []).append((array, unit, cols))
    got, [(_, terms)] = entries_of([0], plan.all)
    return finish(plan, tables, got, terms)


def middle_names(n):
    return [f"middle{i}" for i in range(n)]


def schedule(extra):
    moves = []

    def move(bit, which, **fixed):
        moves.append((bit, which, fixed))

    def thin(which, **fixed):
        for i, n in enumerate(extra):
            move(n, which, core=0, first=0, then=0, **{m: 0 for m in extra[:i]}, **fixed)

    end = dict(core=0, first=0, then=0, **{n: 0 for n in extra})
    move("core", "left", far=1)
    move("core", "right", far=1)
    move("core", "whole", far=0, near=1)
    move("core", "whole", far=0, near=0)
    move("first", "left", core=0, far=1)
    move("first", "right", core=0, far=1)
    move("near", "whole", core=0, far=0, first=1)
    move("then", "whole", core=0, far=0, near=1, first=0)
    move("then", "left", core=0, far=1, first=0)
    thin("left", far=1)
    thin("whole", far=0, near=1)
    move("near", "whole", far=0, **end)
    move("then", "right", core=0, far=1, first=0)
    thin("right", far=1)
    move("near", "left", far=1, **end)
    move("first", "whole", core=0, far=0, near=0)
    move("near", "right", far=1, **end)
    move("far", "left", near=0, **end)
    move("then", "whole", core=0, far=0, near=0, first=0)
    thin("whole", far=0, near=0)
    move("far", "right", near=0, **end)
    return moves


def solution(mesh):
    placed = (P(AXES, None), P(AXES, None), P(AXES))

    return jax.shard_map(
        per_device,
        mesh=mesh,
        in_specs=placed,
        out_specs=(P(AXES, None), P(AXES)),
        check_vma=False,
    )
```

```python
import functools

import jax
import jax.numpy as jnp
from jax import lax
from jax.experimental import pallas as pl
from jax.experimental.pallas import tpu as pltpu
from jax.sharding import PartitionSpec as P


KEYS = 4096
LANES = 128
SUB = 8
TABLES = 3
AXES = ("dom", "rep")
VMEM = pl.BlockSpec(memory_space=pltpu.VMEM)


def bits_of(size):
    return [b for b in range(size.bit_length() - 1)]


class Plan:
    def __init__(self, n_dom, n_rep, rows, width):
        self.devices = n_dom * n_rep
        self.block = KEYS // self.devices
        self.span = KEYS // n_dom
        self.tiles = width // LANES
        self.rows = rows
        self.group = SUB * (self.tiles + 1)
        self.groups = self.block // SUB
        self.part = self.block * self.tiles
        self.unit = self.part + SUB
        self.all = tuple(range(self.tiles))
        rep = bits_of(n_rep)
        dom = [len(rep) + b for b in bits_of(n_dom)]
        self.core, self.second, self.third, self.near, *self.middle, self.far = dom + rep
        head = [self.core, self.far, self.near]
        self.even = [*head, self.second, self.third, *self.middle]
        self.odd = [*head, self.third, self.second, *self.middle]

    def blocks(self, **fixed):
        names = ["core", "far", "near", "first", "then"]
        names += [f"middle{i}" for i in range(len(self.middle))]
        weight = {n: 1 << at for at, n in enumerate(reversed(names))}
        return [
            b
            for b in range(self.devices)
            if all(bool(b & weight[n]) == bool(v) for n, v in fixed.items())
        ], weight

    def payload(self, blocks, cols, counted):
        lines = self.block * len(cols) + (SUB if counted else 0)
        return jax.ShapeDtypeStruct((len(blocks), lines, LANES), jnp.float32)

    def virtual(self, place, order):
        out = jnp.zeros_like(place)
        for at, bit in enumerate(reversed(order)):
            out = out | (((place >> bit) & 1) << at)
        return out

    def pairs(self, even_bit, odd_bit):
        odd = 1 << self.core
        return [
            (i, i ^ (1 << (odd_bit if i & odd else even_bit))) for i in range(self.devices)
        ]


def sum_block(plan, tables, base, out, at, arrived, cols, counted):
    first = pl.multiple_of(base * (plan.groups * plan.group), SUB)

    def table_sum(g, t):
        d = pl.ds(first + g * plan.group + t * SUB, SUB)
        total = tables[0][d, :]
        for table in tables[1:]:
            total = total + table[d, :]
        return total

    for g in range(plan.groups):
        for t in cols:
            total = table_sum(g, t)
            for ref, where, own in arrived:
                if t in own:
                    line = (g * len(own) + own.index(t)) * SUB
                    total = total + ref[where, pl.ds(line, SUB), :]
            line = (g * len(cols) + cols.index(t)) * SUB
            out[at, pl.ds(line, SUB), :] = total
    if counted:
        row = lax.broadcasted_iota(jnp.int32, (SUB, LANES), 0)
        lane = lax.broadcasted_iota(jnp.int32, (SUB, LANES), 1)
        counts = jnp.zeros((SUB, LANES), jnp.float32)
        for g in range(plan.groups):
            counts = jnp.where(lane == row + g * SUB, table_sum(g, plan.tiles), counts)
        total = jnp.broadcast_to(jnp.sum(counts, axis=0, keepdims=True), (SUB, LANES))
        for ref, where, own in arrived:
            line = plan.block * len(own)
            if ref.shape[1] > line:
                total = total + ref[where, pl.ds(line, SUB), :]
        out[at, pl.ds(plan.block * len(cols), SUB), :] = total


def table_kernel(plan, n_rep, entries, cols, counted, owner, offset, facts, sent, *rest):
    tables = rest[:TABLES]
    buf, owner_v, offset_v, addr_v, addr_s, same_v, same_s, sem, small = rest[TABLES:]
    n = plan.rows // LANES
    half = n // 2
    lines = LANES * plan.tiles

    def fetch(i):
        d = pl.ds(i * lines, lines)
        return pltpu.make_async_copy(facts.at[d], buf.at[d], sem.at[i])

    copies = [
        pltpu.make_async_copy(owner, owner_v, small.at[0]),
        pltpu.make_async_copy(offset, offset_v, small.at[1]),
    ]
    for copy in copies:
        copy.start()
    for i in range(half):
        fetch(i).start()
        fetch(half + i).start()

    def zero(refs):
        step = 4 * SUB * SUB

        def body(i, _):
            for t in refs:
                t[pl.ds(pl.multiple_of(i * step, step), step), :] = jnp.zeros(
                    (step, LANES), jnp.float32
                )
            return 0

        lax.fori_loop(0, refs[0].shape[0] // step, body, 0)

    zero(tables[: TABLES // 2])
    for copy in copies:
        copy.wait()
    me = lax.axis_index(AXES[0]) * n_rep + lax.axis_index(AXES[1])
    key = owner_v[...] * plan.span + offset_v[...]
    shift = plan.block.bit_length() - 1
    owner_core = (key >> (shift + plan.core)) & 1
    place = (key >> shift) ^ me
    place = jnp.where(
        owner_core == 1, plan.virtual(place, plan.odd), plan.virtual(place, plan.even)
    )
    key = (place << shift) | (key & (plan.block - 1))
    addr = (key >> 3) * plan.group + (key & (SUB - 1))
    addr_v[...] = addr
    same_v[...] = jnp.where(addr[:half] == addr[half:], 1.0, 0.0)
    copies = [
        pltpu.make_async_copy(addr_v, addr_s, small.at[2]),
        pltpu.make_async_copy(same_v, same_s, small.at[3]),
    ]
    for copy in copies:
        copy.start()
    zero(tables[TABLES // 2 :])
    for copy in copies:
        copy.wait()

    width = plan.tiles + 1
    counted_line = lax.broadcasted_iota(jnp.int32, (width, LANES), 0) == plan.tiles

    def fact(i, j):
        at = pl.ds(i * lines + (j // SUB) * plan.tiles * SUB + j % SUB, width, stride=SUB)
        return jnp.where(counted_line, 1.0, buf[at, :])

    def add_rows(i, _):
        fetch(i).wait()
        fetch(half + i).wait()
        for j in range(LANES):
            table = tables[j % TABLES]
            one = pl.ds(addr_s[i, j], width, stride=SUB)
            two = pl.ds(addr_s[half + i, j], width, stride=SUB)
            row_one, row_two = fact(i, j), fact(half + i, j)
            old_one = table[one, :]
            old_two = table[two, :]
            table[one, :] = old_one + row_one
            table[two, :] = old_two + (row_two + same_s[i, j] * row_one)
        return 0

    lax.fori_loop(0, half, add_rows, 0)

    send_runs(plan, tables, (), sent, entries, cols, counted)


def make_table(plan, n_rep, owner, offset, facts, blocks, cols, counted):
    rows = plan.rows
    view = facts.reshape(rows // SUB, SUB, plan.tiles, LANES).transpose(0, 2, 1, 3)
    view = view.reshape(rows * plan.tiles, LANES)
    lanes = (rows // LANES, LANES)
    half = (rows // LANES // 2, LANES)
    far = [
        pltpu.with_memory_space_constraint(x, pltpu.HBM)
        for x in (owner.reshape(lanes), offset.reshape(lanes), view)
    ]
    hbm = pl.BlockSpec(memory_space=pltpu.HBM)
    table = jax.ShapeDtypeStruct((KEYS // SUB * plan.group, LANES), jnp.float32)
    return pl.pallas_call(
        functools.partial(
            table_kernel, plan, n_rep, [(b, ()) for b in blocks], cols, counted
        ),
        out_shape=[plan.payload(blocks, cols, counted)]
        + [table] * TABLES,
        in_specs=[hbm, hbm, hbm],
        out_specs=[VMEM] * (1 + TABLES),
        scratch_shapes=[
            pltpu.VMEM((rows * plan.tiles + 2 * SUB, LANES), jnp.float32),
            pltpu.VMEM(lanes, jnp.int32),
            pltpu.VMEM(lanes, jnp.int32),
            pltpu.VMEM(lanes, jnp.int32),
            pltpu.SMEM(lanes, jnp.int32),
            pltpu.VMEM(half, jnp.float32),
            pltpu.SMEM(half, jnp.float32),
            pltpu.SemaphoreType.DMA((rows // LANES,)),
            pltpu.SemaphoreType.DMA((4,)),
        ],
        compiler_params=pltpu.CompilerParams(vmem_limit_bytes=12 << 20),
        name="make_table",
    )(*far)


def send_runs(plan, tables, arrays, out, entries, cols, counted):
    def follows(a, b):
        return b[0] == a[0] + 1 and [(k, u + 1, o) for k, u, o in a[1]] == list(b[1])

    start = 0
    while start < len(entries):
        end = start + 1
        while end < len(entries) and follows(entries[end - 1], entries[end]):
            end += 1
        block, terms = entries[start]

        def body(i, _):
            arrived = [(arrays[k], u + i, own) for k, u, own in terms]
            sum_block(plan, tables, block + i, out, start + i, arrived, cols, counted)
            return 0

        lax.fori_loop(0, end - start, body, 0)
        start = end


def send_kernel(plan, n_got, entries, cols, counted, *refs):
    tables, got, out = refs[:TABLES], refs[TABLES : TABLES + n_got], refs[-1]
    send_runs(plan, tables, got, out, entries, cols, counted)


def send_blocks(plan, tables, got, entries, cols, counted):
    n = len(tables) + len(got)
    return pl.pallas_call(
        functools.partial(send_kernel, plan, len(got), entries, cols, counted),
        out_shape=plan.payload(entries, cols, counted),
        in_specs=[VMEM] * n,
        out_specs=VMEM,
        compiler_params=pltpu.CompilerParams(vmem_limit_bytes=4 << 20),
        name="send_blocks",
    )(*tables, *got)


def finish_kernel(plan, n_got, terms, *refs):
    tables, got = refs[:TABLES], refs[TABLES : TABLES + n_got]
    means, counts, total = refs[TABLES + n_got :]
    arrived = [(got[k], u, own) for k, u, own in terms]
    sum_block(plan, tables, 0, total, 0, arrived, plan.all, True)
    row = total[0, pl.ds(plan.part, 1), :]
    counts[...] = row[:, : plan.block]
    shape = (plan.block, LANES)
    diagonal = lax.broadcasted_iota(jnp.int32, shape, 0) == lax.broadcasted_iota(
        jnp.int32, shape, 1
    )
    column = jnp.sum(jnp.where(diagonal, row, 0.0), axis=1, keepdims=True)
    column = jnp.maximum(column, 1.0)
    for g in range(plan.groups):
        for t in range(plan.tiles):
            means[g * SUB : (g + 1) * SUB, t * LANES : (t + 1) * LANES] = (
                total[0, pl.ds((g * plan.tiles + t) * SUB, SUB), :]
                / column[g * SUB : (g + 1) * SUB, :]
            )


def finish(plan, tables, got, terms):
    means, counts = pl.pallas_call(
        functools.partial(finish_kernel, plan, len(got), terms),
        out_shape=[
            jax.ShapeDtypeStruct((plan.block, plan.tiles * LANES), jnp.float32),
            jax.ShapeDtypeStruct((1, plan.block), jnp.float32),
        ],
        in_specs=[VMEM] * (len(tables) + len(got)),
        out_specs=[VMEM] * 2,
        scratch_shapes=[pltpu.VMEM((1, plan.unit, LANES), jnp.float32)],
        compiler_params=pltpu.CompilerParams(vmem_limit_bytes=4 << 20),
        name="finish",
    )(*tables, *got)
    return means, counts.reshape(plan.block)


def per_device(facts, row_owner, key_offset):
    n_dom, n_rep = lax.axis_size("dom"), lax.axis_size("rep")
    plan = Plan(n_dom, n_rep, *facts.shape)
    pairs = {
        "core": (plan.core, plan.core),
        "first": (plan.second, plan.third),
        "then": (plan.third, plan.second),
        "near": (plan.near, plan.near),
        "far": (plan.far, plan.far),
    }
    extra = middle_names(len(plan.middle))
    pairs |= {n: (bit, bit) for n, bit in zip(extra, plan.middle)}
    arrived = {}
    tables = None

    def entries_of(blocks, cols):
        got, entries = [], []
        for b in blocks:
            terms = []
            for array, unit, own in arrived.get(b, []):
                if not set(own) & set(cols):
                    continue
                at = [i for i, g in enumerate(got) if g is array]
                if not at:
                    at = [len(got)]
                    got.append(array)
                terms.append((at[0], unit, own))
            entries.append((b, tuple(terms)))
        return got, entries

    parts = {"whole": (plan.all, True)}
    for bit, which, fixed in schedule(extra):
        cols, counted = parts[which]
        blocks, weight = plan.blocks(**{bit: 1}, **fixed)
        if tables is None:
            sent, *tables = make_table(
                plan, n_rep, row_owner[:, 0], key_offset, facts, blocks, cols, counted
            )
        else:
            got, entries = entries_of(blocks, cols)
            sent = send_blocks(plan, tables, got, entries, cols, counted)
        array = lax.ppermute(sent, AXES, plan.pairs(*pairs[bit]))
        for unit, b in enumerate(blocks):
            arrived.setdefault(b - weight[bit], []).append((array, unit, cols))
    got, [(_, terms)] = entries_of([0], plan.all)
    return finish(plan, tables, got, terms)


def middle_names(n):
    return [f"middle{i}" for i in range(n)]


def schedule(extra):
    moves = []

    def move(bit, **fixed):
        moves.append((bit, "whole", fixed))

    def then(**fixed):
        move("then", core=0, first=0, **fixed)
        for i, n in enumerate(extra):
            move(n, core=0, first=0, then=0, **{m: 0 for m in extra[:i]}, **fixed)

    end = dict(core=0, first=0, then=0, **{n: 0 for n in extra})
    move("core", far=1, first=1)
    move("core", far=1, first=0)
    move("core", far=0, near=1)
    move("core", far=0, near=0)
    move("first", core=0, far=1, near=1)
    move("first", core=0, far=1, near=0)
    move("near", core=0, far=0, first=1)
    then(far=1, near=1)
    then(far=0, near=1)
    then(far=1, near=0)
    move("near", far=1, **end)
    move("first", core=0, far=0, near=0)
    move("near", far=0, **end)
    move("far", near=0, **end)
    then(far=0, near=0)
    return moves


def solution(mesh):
    placed = (P(AXES, None), P(AXES, None), P(AXES))

    return jax.shard_map(
        per_device,
        mesh=mesh,
        in_specs=placed,
        out_specs=(P(AXES, None), P(AXES)),
        check_vma=False,
    )
```

```python
import functools

import jax
import jax.numpy as jnp
from jax import lax
from jax.experimental import pallas as pl
from jax.experimental.pallas import tpu as pltpu
from jax.sharding import PartitionSpec as P


KEYS = 4096
LANES = 128
SUB = 8
TABLES = 3
AXES = ("dom", "rep")
VMEM = pl.BlockSpec(memory_space=pltpu.VMEM)


def bits_of(size):
    return [b for b in range(size.bit_length() - 1)]


class Plan:
    def __init__(self, n_dom, n_rep, rows, width):
        self.devices = n_dom * n_rep
        self.block = KEYS // self.devices
        self.span = KEYS // n_dom
        self.tiles = width // LANES
        self.rows = rows
        self.group = SUB * (self.tiles + 1)
        self.groups = self.block // SUB
        self.part = self.block * self.tiles
        self.unit = self.part + SUB
        self.all = tuple(range(self.tiles))
        rep = bits_of(n_rep)
        dom = [len(rep) + b for b in bits_of(n_dom)]
        self.core, self.second, self.third, self.near, *self.middle, self.far = dom + rep
        head = [self.core, self.far, self.near]
        self.even = [*head, self.second, self.third, *self.middle]
        self.odd = [*head, self.third, self.second, *self.middle]

    def blocks(self, **fixed):
        names = ["core", "far", "near", "first", "then"]
        names += [f"middle{i}" for i in range(len(self.middle))]
        weight = {n: 1 << at for at, n in enumerate(reversed(names))}
        return [
            b
            for b in range(self.devices)
            if all(bool(b & weight[n]) == bool(v) for n, v in fixed.items())
        ], weight

    def payload(self, blocks, cols, counted):
        lines = self.block * len(cols) + (SUB if counted else 0)
        return jax.ShapeDtypeStruct((len(blocks), lines, LANES), jnp.float32)

    def virtual(self, place, order):
        out = jnp.zeros_like(place)
        for at, bit in enumerate(reversed(order)):
            out = out | (((place >> bit) & 1) << at)
        return out

    def pairs(self, even_bit, odd_bit):
        odd = 1 << self.core
        return [
            (i, i ^ (1 << (odd_bit if i & odd else even_bit))) for i in range(self.devices)
        ]


def sum_block(plan, tables, base, out, at, arrived, cols, counted):
    first = pl.multiple_of(base * (plan.groups * plan.group), SUB)

    def table_sum(g, t):
        d = pl.ds(first + g * plan.group + t * SUB, SUB)
        total = tables[0][d, :]
        for table in tables[1:]:
            total = total + table[d, :]
        return total

    for g in range(plan.groups):
        for t in cols:
            total = table_sum(g, t)
            for ref, where, own in arrived:
                if t in own:
                    line = (g * len(own) + own.index(t)) * SUB
                    total = total + ref[where, pl.ds(line, SUB), :]
            line = (g * len(cols) + cols.index(t)) * SUB
            out[at, pl.ds(line, SUB), :] = total
    if counted:
        row = lax.broadcasted_iota(jnp.int32, (SUB, LANES), 0)
        lane = lax.broadcasted_iota(jnp.int32, (SUB, LANES), 1)
        counts = jnp.zeros((SUB, LANES), jnp.float32)
        for g in range(plan.groups):
            counts = jnp.where(lane == row + g * SUB, table_sum(g, plan.tiles), counts)
        total = jnp.broadcast_to(jnp.sum(counts, axis=0, keepdims=True), (SUB, LANES))
        for ref, where, own in arrived:
            line = plan.block * len(own)
            if ref.shape[1] > line:
                total = total + ref[where, pl.ds(line, SUB), :]
        out[at, pl.ds(plan.block * len(cols), SUB), :] = total


def table_kernel(plan, n_rep, entries, cols, counted, owner, offset, facts, sent, *rest):
    tables = rest[:TABLES]
    buf, owner_v, offset_v, addr_v, one_s, two_s, same_v, same_s, sem, small = rest[TABLES:]
    n = plan.rows // LANES
    half = n // 2
    lines = LANES * plan.tiles

    def fetch(i):
        d = pl.ds(i * lines, lines)
        return pltpu.make_async_copy(facts.at[d], buf.at[d], sem.at[i])

    copies = [
        pltpu.make_async_copy(owner, owner_v, small.at[0]),
        pltpu.make_async_copy(offset, offset_v, small.at[1]),
    ]
    for copy in copies:
        copy.start()
    for i in range(half):
        fetch(i).start()
        fetch(half + i).start()

    def zero(refs):
        step = 4 * SUB * SUB

        def body(i, _):
            for t in refs:
                t[pl.ds(pl.multiple_of(i * step, step), step), :] = jnp.zeros(
                    (step, LANES), jnp.float32
                )
            return 0

        lax.fori_loop(0, refs[0].shape[0] // step, body, 0)

    zero(tables[: (TABLES + 1) // 2])
    for copy in copies:
        copy.wait()
    me = lax.axis_index(AXES[0]) * n_rep + lax.axis_index(AXES[1])
    key = owner_v[...] * plan.span + offset_v[...]
    shift = plan.block.bit_length() - 1
    owner_core = (key >> (shift + plan.core)) & 1
    place = (key >> shift) ^ me
    place = jnp.where(
        owner_core == 1, plan.virtual(place, plan.odd), plan.virtual(place, plan.even)
    )
    key = (place << shift) | (key & (plan.block - 1))
    addr = (key >> 3) * plan.group + (key & (SUB - 1))
    addr_v[...] = addr
    same_v[...] = jnp.where(addr[:half] == addr[half:], 1.0, 0.0)
    copies = [
        pltpu.make_async_copy(addr_v.at[pl.ds(0, half)], one_s, small.at[2]),
        pltpu.make_async_copy(addr_v.at[pl.ds(half, half)], two_s, small.at[3]),
        pltpu.make_async_copy(same_v, same_s, small.at[4]),
    ]
    for copy in copies:
        copy.start()
    zero(tables[(TABLES + 1) // 2 :])
    for copy in copies:
        copy.wait()

    width = plan.tiles + 1
    line = lax.broadcasted_iota(jnp.int32, (SUB, LANES), 0)

    def eight_facts(i, g):
        base = i * lines + g * (SUB * plan.tiles)
        return [
            buf[pl.ds(pl.multiple_of(base + t * SUB, SUB), SUB), :] for t in range(plan.tiles)
        ]

    def fact(parts, j):
        row = jnp.ones((SUB, LANES), jnp.float32)
        for t, part in enumerate(parts):
            row = jnp.where(line == t, pltpu.roll(part, (t - j) % SUB, 0), row)
        return row[:width]

    def add_rows(i, _):
        fetch(i).wait()
        fetch(half + i).wait()
        for j in range(LANES):
            if j % SUB == 0:
                first, then = eight_facts(i, j // SUB), eight_facts(half + i, j // SUB)
            table = tables[j % TABLES]
            one = pl.ds(one_s[i, j], width, stride=SUB)
            two = pl.ds(two_s[i, j], width, stride=SUB)
            row_one, row_two = fact(first, j % SUB), fact(then, j % SUB)
            old_one = table[one, :]
            old_two = table[two, :]
            table[one, :] = old_one + row_one
            table[two, :] = old_two + (row_two + same_s[i, j] * row_one)
        return 0

    lax.fori_loop(0, half, add_rows, 0)

    send_runs(plan, tables, (), sent, entries, cols, counted)


def make_table(plan, n_rep, owner, offset, facts, blocks, cols, counted):
    rows = plan.rows
    view = facts.reshape(rows // SUB, SUB, plan.tiles, LANES).transpose(0, 2, 1, 3)
    view = view.reshape(rows * plan.tiles, LANES)
    lanes = (rows // LANES, LANES)
    half = (rows // LANES // 2, LANES)
    far = [
        pltpu.with_memory_space_constraint(x, pltpu.HBM)
        for x in (owner.reshape(lanes), offset.reshape(lanes), view)
    ]
    hbm = pl.BlockSpec(memory_space=pltpu.HBM)
    table = jax.ShapeDtypeStruct((KEYS // SUB * plan.group, LANES), jnp.float32)
    return pl.pallas_call(
        functools.partial(
            table_kernel, plan, n_rep, [(b, ()) for b in blocks], cols, counted
        ),
        out_shape=[plan.payload(blocks, cols, counted)]
        + [table] * TABLES,
        in_specs=[hbm, hbm, hbm],
        out_specs=[VMEM] * (1 + TABLES),
        scratch_shapes=[
            pltpu.VMEM((rows * plan.tiles + 2 * SUB, LANES), jnp.float32),
            pltpu.VMEM(lanes, jnp.int32),
            pltpu.VMEM(lanes, jnp.int32),
            pltpu.VMEM(lanes, jnp.int32),
            pltpu.SMEM(half, jnp.int32),
            pltpu.SMEM(half, jnp.int32),
            pltpu.VMEM(half, jnp.float32),
            pltpu.SMEM(half, jnp.float32),
            pltpu.SemaphoreType.DMA((rows // LANES,)),
            pltpu.SemaphoreType.DMA((5,)),
        ],
        compiler_params=pltpu.CompilerParams(vmem_limit_bytes=12 << 20),
        name="make_table",
    )(*far)


def send_runs(plan, tables, arrays, out, entries, cols, counted):
    def follows(a, b):
        return b[0] == a[0] + 1 and [(k, u + 1, o) for k, u, o in a[1]] == list(b[1])

    start = 0
    while start < len(entries):
        end = start + 1
        while end < len(entries) and follows(entries[end - 1], entries[end]):
            end += 1
        block, terms = entries[start]

        def body(i, _):
            arrived = [(arrays[k], u + i, own) for k, u, own in terms]
            sum_block(plan, tables, block + i, out, start + i, arrived, cols, counted)
            return 0

        lax.fori_loop(0, end - start, body, 0)
        start = end


def send_kernel(plan, n_got, entries, cols, counted, *refs):
    tables, got, out = refs[:TABLES], refs[TABLES : TABLES + n_got], refs[-1]
    send_runs(plan, tables, got, out, entries, cols, counted)


def send_blocks(plan, tables, got, entries, cols, counted):
    n = len(tables) + len(got)
    return pl.pallas_call(
        functools.partial(send_kernel, plan, len(got), entries, cols, counted),
        out_shape=plan.payload(entries, cols, counted),
        in_specs=[VMEM] * n,
        out_specs=VMEM,
        compiler_params=pltpu.CompilerParams(vmem_limit_bytes=4 << 20),
        name="send_blocks",
    )(*tables, *got)


def finish_kernel(plan, n_got, terms, *refs):
    tables, got = refs[:TABLES], refs[TABLES : TABLES + n_got]
    means, counts, total = refs[TABLES + n_got :]
    arrived = [(got[k], u, own) for k, u, own in terms]
    sum_block(plan, tables, 0, total, 0, arrived, plan.all, True)
    row = total[0, pl.ds(plan.part, 1), :]
    counts[...] = row[:, : plan.block]
    shape = (plan.block, LANES)
    diagonal = lax.broadcasted_iota(jnp.int32, shape, 0) == lax.broadcasted_iota(
        jnp.int32, shape, 1
    )
    column = jnp.sum(jnp.where(diagonal, row, 0.0), axis=1, keepdims=True)
    column = jnp.maximum(column, 1.0)
    for g in range(plan.groups):
        for t in range(plan.tiles):
            means[g * SUB : (g + 1) * SUB, t * LANES : (t + 1) * LANES] = (
                total[0, pl.ds((g * plan.tiles + t) * SUB, SUB), :]
                / column[g * SUB : (g + 1) * SUB, :]
            )


def finish(plan, tables, got, terms):
    means, counts = pl.pallas_call(
        functools.partial(finish_kernel, plan, len(got), terms),
        out_shape=[
            jax.ShapeDtypeStruct((plan.block, plan.tiles * LANES), jnp.float32),
            jax.ShapeDtypeStruct((1, plan.block), jnp.float32),
        ],
        in_specs=[VMEM] * (len(tables) + len(got)),
        out_specs=[VMEM] * 2,
        scratch_shapes=[pltpu.VMEM((1, plan.unit, LANES), jnp.float32)],
        compiler_params=pltpu.CompilerParams(vmem_limit_bytes=4 << 20),
        name="finish",
    )(*tables, *got)
    return means, counts.reshape(plan.block)


def per_device(facts, row_owner, key_offset):
    n_dom, n_rep = lax.axis_size("dom"), lax.axis_size("rep")
    plan = Plan(n_dom, n_rep, *facts.shape)
    pairs = {
        "core": (plan.core, plan.core),
        "first": (plan.second, plan.third),
        "then": (plan.third, plan.second),
        "near": (plan.near, plan.near),
        "far": (plan.far, plan.far),
    }
    extra = middle_names(len(plan.middle))
    pairs |= {n: (bit, bit) for n, bit in zip(extra, plan.middle)}
    arrived = {}
    tables = None

    def entries_of(blocks, cols):
        got, entries = [], []
        for b in blocks:
            terms = []
            for array, unit, own in arrived.get(b, []):
                if not set(own) & set(cols):
                    continue
                at = [i for i, g in enumerate(got) if g is array]
                if not at:
                    at = [len(got)]
                    got.append(array)
                terms.append((at[0], unit, own))
            entries.append((b, tuple(terms)))
        return got, entries

    cols, counted = plan.all, True
    for bit, fixed in schedule(extra):
        blocks, weight = plan.blocks(**{bit: 1}, **fixed)
        if tables is None:
            sent, *tables = make_table(
                plan, n_rep, row_owner[:, 0], key_offset, facts, blocks, cols, counted
            )
        else:
            got, entries = entries_of(blocks, cols)
            sent = send_blocks(plan, tables, got, entries, cols, counted)
        array = lax.ppermute(sent, AXES, plan.pairs(*pairs[bit]))
        for unit, b in enumerate(blocks):
            arrived.setdefault(b - weight[bit], []).append((array, unit, cols))
    got, [(_, terms)] = entries_of([0], plan.all)
    return finish(plan, tables, got, terms)


def middle_names(n):
    return [f"middle{i}" for i in range(n)]


def schedule(extra):
    moves = []

    def move(bit, **fixed):
        moves.append((bit, fixed))

    def then(**fixed):
        move("then", core=0, first=0, **fixed)
        for i, n in enumerate(extra):
            move(n, core=0, first=0, then=0, **{m: 0 for m in extra[:i]}, **fixed)

    end = dict(core=0, first=0, then=0, **{n: 0 for n in extra})
    move("core", far=1, first=1)
    move("core", far=1, first=0)
    move("core", far=0, near=1)
    move("core", far=0, near=0)
    move("first", core=0, far=1, then=1)
    move("first", core=0, far=1, then=0)
    move("near", core=0, far=0, first=1, then=1)
    move("near", core=0, far=0, first=1, then=0)
    then(far=1, near=1)
    then(far=1, near=0)
    then(far=0, near=1)
    move("near", far=1, **end)
    move("first", core=0, far=0, near=0, then=1)
    move("first", core=0, far=0, near=0, then=0)
    move("near", far=0, **end)
    move("far", near=0, **end)
    then(far=0, near=0)
    return moves


def solution(mesh):
    placed = (P(AXES, None), P(AXES, None), P(AXES))

    return jax.shard_map(
        per_device,
        mesh=mesh,
        in_specs=placed,
        out_specs=(P(AXES, None), P(AXES)),
        check_vma=False,
    )
```

```python
import functools

import jax
import jax.numpy as jnp
from jax import lax
from jax.experimental import pallas as pl
from jax.experimental.pallas import tpu as pltpu
from jax.sharding import PartitionSpec as P


KEYS = 4096
LANES = 128
SUB = 8
TABLES = 3
AXES = ("dom", "rep")
VMEM = pl.BlockSpec(memory_space=pltpu.VMEM)


def bits_of(size):
    return [b for b in range(size.bit_length() - 1)]


class Plan:
    def __init__(self, n_dom, n_rep, rows, width):
        self.devices = n_dom * n_rep
        self.block = KEYS // self.devices
        self.span = KEYS // n_dom
        self.tiles = width // LANES
        self.rows = rows
        self.group = SUB * (self.tiles + 1)
        self.groups = self.block // SUB
        self.part = self.block * self.tiles
        self.all = tuple(range(self.tiles))
        rep = bits_of(n_rep)
        dom = [len(rep) + b for b in bits_of(n_dom)]
        self.core, self.second, self.third, self.near, *self.middle, self.far = dom + rep
        head = [self.core, self.far, self.near]
        self.even = [*head, self.second, self.third, *self.middle]
        self.odd = [*head, self.third, self.second, *self.middle]

    def blocks(self, **fixed):
        names = ["core", "far", "near", "first", "then"]
        names += [f"middle{i}" for i in range(len(self.middle))]
        weight = {n: 1 << at for at, n in enumerate(reversed(names))}
        return [
            b
            for b in range(self.devices)
            if all(bool(b & weight[n]) == bool(v) for n, v in fixed.items())
        ], weight

    def payload(self, blocks, cols, counted):
        lines = self.block * len(cols) + (SUB if counted else 0)
        return jax.ShapeDtypeStruct((len(blocks), lines, LANES), jnp.float32)

    def virtual(self, place, order):
        out = jnp.zeros_like(place)
        for at, bit in enumerate(reversed(order)):
            out = out | (((place >> bit) & 1) << at)
        return out

    def pairs(self, even_bit, odd_bit):
        odd = 1 << self.core
        return [
            (i, i ^ (1 << (odd_bit if i & odd else even_bit))) for i in range(self.devices)
        ]


def sum_block(plan, tables, base, out, at, arrived, cols, counted):
    first = pl.multiple_of(base * (plan.groups * plan.group), SUB)

    def table_sum(g, t):
        d = pl.ds(first + g * plan.group + t * SUB, SUB)
        total = tables[0][d, :]
        for table in tables[1:]:
            total = total + table[d, :]
        return total

    for g in range(plan.groups):
        for t in cols:
            total = table_sum(g, t)
            for ref, where, own in arrived:
                if t in own:
                    line = (g * len(own) + own.index(t)) * SUB
                    total = total + ref[where, pl.ds(line, SUB), :]
            line = (g * len(cols) + cols.index(t)) * SUB
            out[at, pl.ds(line, SUB), :] = total
    if counted:
        row = lax.broadcasted_iota(jnp.int32, (SUB, LANES), 0)
        lane = lax.broadcasted_iota(jnp.int32, (SUB, LANES), 1)
        counts = jnp.zeros((SUB, LANES), jnp.float32)
        for g in range(plan.groups):
            counts = jnp.where(lane == row + g * SUB, table_sum(g, plan.tiles), counts)
        total = jnp.broadcast_to(jnp.sum(counts, axis=0, keepdims=True), (SUB, LANES))
        for ref, where, own in arrived:
            line = plan.block * len(own)
            if ref.shape[1] > line:
                total = total + ref[where, pl.ds(line, SUB), :]
        out[at, pl.ds(plan.block * len(cols), SUB), :] = total


def table_kernel(plan, n_rep, entries, cols, counted, owner, offset, facts, sent, *rest):
    tables = rest[:TABLES]
    buf, owner_v, offset_v, addr_v, one_s, two_s, same_v, same_s, sem, small = rest[TABLES:]
    n = plan.rows // LANES
    half = n // 2
    lines = LANES * plan.tiles

    def fetch(i):
        d = pl.ds(i * lines, lines)
        return pltpu.make_async_copy(facts.at[d], buf.at[d], sem.at[i])

    copies = [
        pltpu.make_async_copy(owner, owner_v, small.at[0]),
        pltpu.make_async_copy(offset, offset_v, small.at[1]),
    ]
    for copy in copies:
        copy.start()
    for i in range(half):
        fetch(i).start()
        fetch(half + i).start()

    def zero(refs):
        step = 4 * SUB * SUB

        def body(i, _):
            for t in refs:
                t[pl.ds(pl.multiple_of(i * step, step), step), :] = jnp.zeros(
                    (step, LANES), jnp.float32
                )
            return 0

        lax.fori_loop(0, refs[0].shape[0] // step, body, 0)

    zero(tables[: (TABLES + 1) // 2])
    for copy in copies:
        copy.wait()
    me = lax.axis_index(AXES[0]) * n_rep + lax.axis_index(AXES[1])
    key = owner_v[...] * plan.span + offset_v[...]
    shift = plan.block.bit_length() - 1
    owner_core = (key >> (shift + plan.core)) & 1
    place = (key >> shift) ^ me
    place = jnp.where(
        owner_core == 1, plan.virtual(place, plan.odd), plan.virtual(place, plan.even)
    )
    key = (place << shift) | (key & (plan.block - 1))
    addr = (key >> 3) * plan.group + (key & (SUB - 1))
    addr_v[...] = addr
    same_v[...] = jnp.where(addr[:half] == addr[half:], 1.0, 0.0)
    copies = [
        pltpu.make_async_copy(addr_v.at[pl.ds(0, half)], one_s, small.at[2]),
        pltpu.make_async_copy(addr_v.at[pl.ds(half, half)], two_s, small.at[3]),
        pltpu.make_async_copy(same_v, same_s, small.at[4]),
    ]
    for copy in copies:
        copy.start()
    zero(tables[(TABLES + 1) // 2 :])
    for copy in copies:
        copy.wait()

    width = plan.tiles + 1
    line = lax.broadcasted_iota(jnp.int32, (SUB, LANES), 0)

    def eight_facts(i, g):
        base = i * lines + g * (SUB * plan.tiles)
        return [
            buf[pl.ds(pl.multiple_of(base + t * SUB, SUB), SUB), :] for t in range(plan.tiles)
        ]

    def fact(parts, j):
        row = jnp.ones((SUB, LANES), jnp.float32)
        for t, part in enumerate(parts):
            row = jnp.where(line == t, pltpu.roll(part, (t - j) % SUB, 0), row)
        return row[:width]

    def add_rows(i, _):
        fetch(i).wait()
        fetch(half + i).wait()
        for j in range(LANES):
            if j % SUB == 0:
                first, then = eight_facts(i, j // SUB), eight_facts(half + i, j // SUB)
            table = tables[j % TABLES]
            one = pl.ds(one_s[i, j], width, stride=SUB)
            two = pl.ds(two_s[i, j], width, stride=SUB)
            row_one, row_two = fact(first, j % SUB), fact(then, j % SUB)
            old_one = table[one, :]
            old_two = table[two, :]
            table[one, :] = old_one + row_one
            table[two, :] = old_two + (row_two + same_s[i, j] * row_one)
        return 0

    lax.fori_loop(0, half, add_rows, 0)

    send_runs(plan, tables, (), sent, entries, cols, counted)


def make_table(plan, n_rep, owner, offset, facts, blocks, cols, counted):
    rows = plan.rows
    view = facts.reshape(rows // SUB, SUB, plan.tiles, LANES).transpose(0, 2, 1, 3)
    view = view.reshape(rows * plan.tiles, LANES)
    lanes = (rows // LANES, LANES)
    half = (rows // LANES // 2, LANES)
    far = [
        pltpu.with_memory_space_constraint(x, pltpu.HBM)
        for x in (owner.reshape(lanes), offset.reshape(lanes), view)
    ]
    hbm = pl.BlockSpec(memory_space=pltpu.HBM)
    table = jax.ShapeDtypeStruct((KEYS // SUB * plan.group, LANES), jnp.float32)
    return pl.pallas_call(
        functools.partial(
            table_kernel, plan, n_rep, [(b, ()) for b in blocks], cols, counted
        ),
        out_shape=[plan.payload(blocks, cols, counted)]
        + [table] * TABLES,
        in_specs=[hbm, hbm, hbm],
        out_specs=[VMEM] * (1 + TABLES),
        scratch_shapes=[
            pltpu.VMEM((rows * plan.tiles + 2 * SUB, LANES), jnp.float32),
            pltpu.VMEM(lanes, jnp.int32),
            pltpu.VMEM(lanes, jnp.int32),
            pltpu.VMEM(lanes, jnp.int32),
            pltpu.SMEM(half, jnp.int32),
            pltpu.SMEM(half, jnp.int32),
            pltpu.VMEM(half, jnp.float32),
            pltpu.SMEM(half, jnp.float32),
            pltpu.SemaphoreType.DMA((rows // LANES,)),
            pltpu.SemaphoreType.DMA((5,)),
        ],
        compiler_params=pltpu.CompilerParams(vmem_limit_bytes=12 << 20),
        name="make_table",
    )(*far)


def send_runs(plan, tables, arrays, out, entries, cols, counted):
    def follows(a, b):
        return b[0] == a[0] + 1 and [(k, u + 1, o) for k, u, o in a[1]] == list(b[1])

    start = 0
    while start < len(entries):
        end = start + 1
        while end < len(entries) and follows(entries[end - 1], entries[end]):
            end += 1
        block, terms = entries[start]

        def body(i, _):
            arrived = [(arrays[k], u + i, own) for k, u, own in terms]
            sum_block(plan, tables, block + i, out, start + i, arrived, cols, counted)
            return 0

        lax.fori_loop(0, end - start, body, 0)
        start = end


def send_kernel(plan, n_got, entries, cols, counted, *refs):
    tables, got, out = refs[:TABLES], refs[TABLES : TABLES + n_got], refs[-1]
    send_runs(plan, tables, got, out, entries, cols, counted)


def send_blocks(plan, tables, got, entries, cols, counted):
    n = len(tables) + len(got)
    return pl.pallas_call(
        functools.partial(send_kernel, plan, len(got), entries, cols, counted),
        out_shape=plan.payload(entries, cols, counted),
        in_specs=[VMEM] * n,
        out_specs=VMEM,
        compiler_params=pltpu.CompilerParams(vmem_limit_bytes=4 << 20),
        name="send_blocks",
    )(*tables, *got)


def finish_kernel(plan, units, *refs):
    got, (means, counts) = refs[: len(units)], refs[len(units) :]

    def total(line, size):
        out = got[0][units[0], pl.ds(line, size), :]
        for ref, unit in zip(got[1:], units[1:]):
            out = out + ref[unit, pl.ds(line, size), :]
        return out

    row = total(plan.part, 1)
    counts[...] = row[:, : plan.block]
    shape = (plan.block, LANES)
    diagonal = lax.broadcasted_iota(jnp.int32, shape, 0) == lax.broadcasted_iota(
        jnp.int32, shape, 1
    )
    column = jnp.sum(jnp.where(diagonal, row, 0.0), axis=1, keepdims=True)
    column = jnp.maximum(column, 1.0)
    for g in range(plan.groups):
        for t in range(plan.tiles):
            means[g * SUB : (g + 1) * SUB, t * LANES : (t + 1) * LANES] = (
                total((g * plan.tiles + t) * SUB, SUB)
                / column[g * SUB : (g + 1) * SUB, :]
            )


def finish(plan, got, units):
    means, counts = pl.pallas_call(
        functools.partial(finish_kernel, plan, units),
        out_shape=[
            jax.ShapeDtypeStruct((plan.block, plan.tiles * LANES), jnp.float32),
            jax.ShapeDtypeStruct((1, plan.block), jnp.float32),
        ],
        in_specs=[VMEM] * len(got),
        out_specs=[VMEM] * 2,
        compiler_params=pltpu.CompilerParams(vmem_limit_bytes=4 << 20),
        name="finish",
    )(*got)
    return means, counts.reshape(plan.block)


def per_device(facts, row_owner, key_offset):
    n_dom, n_rep = lax.axis_size("dom"), lax.axis_size("rep")
    plan = Plan(n_dom, n_rep, *facts.shape)
    pairs = {
        "core": (plan.core, plan.core),
        "first": (plan.second, plan.third),
        "then": (plan.third, plan.second),
        "near": (plan.near, plan.near),
        "far": (plan.far, plan.far),
    }
    extra = middle_names(len(plan.middle))
    pairs |= {n: (bit, bit) for n, bit in zip(extra, plan.middle)}
    arrived = {}
    tables = None

    def entries_of(blocks, cols):
        got, entries = [], []
        for b in blocks:
            terms = []
            for array, unit, own in arrived.get(b, []):
                if not set(own) & set(cols):
                    continue
                at = [i for i, g in enumerate(got) if g is array]
                if not at:
                    at = [len(got)]
                    got.append(array)
                terms.append((at[0], unit, own))
            entries.append((b, tuple(terms)))
        return got, entries

    cols, counted = plan.all, True
    for bit, fixed in schedule(extra):
        blocks, weight = plan.blocks(**{bit: 1}, **fixed)
        if tables is None:
            sent, *tables = make_table(
                plan, n_rep, row_owner[:, 0], key_offset, facts, blocks, cols, counted
            )
        else:
            got, entries = entries_of(blocks, cols)
            sent = send_blocks(plan, tables, got, entries, cols, counted)
        array = lax.ppermute(sent, AXES, plan.pairs(*pairs[bit]))
        for unit, b in enumerate(blocks):
            arrived.setdefault(b - weight[bit], []).append((array, unit, cols))
    late = 2 + len(extra)
    arrived[0], last = arrived[0][:-late], arrived[0][-late:]
    got, entries = entries_of([0], cols)
    early = send_blocks(plan, tables, got, entries, cols, counted)
    arrays = [early] + [array for array, _, _ in last]
    return finish(plan, arrays, [0] + [unit for _, unit, _ in last])


def middle_names(n):
    return [f"middle{i}" for i in range(n)]


def schedule(extra):
    moves = []

    def move(bit, **fixed):
        moves.append((bit, fixed))

    def then(**fixed):
        move("then", core=0, first=0, **fixed)
        for i, n in enumerate(extra):
            move(n, core=0, first=0, then=0, **{m: 0 for m in extra[:i]}, **fixed)

    end = dict(core=0, first=0, then=0, **{n: 0 for n in extra})
    move("core", far=1, first=1)
    move("core", far=1, first=0)
    move("core", far=0, near=1)
    move("first", core=0, far=1, then=1)
    move("first", core=0, far=1, then=0)
    move("core", far=0, near=0)
    move("near", core=0, far=0, first=1, then=1)
    move("near", core=0, far=0, first=1, then=0)
    then(far=1, near=1)
    then(far=1, near=0)
    then(far=0, near=1)
    move("near", far=1, **end)
    move("first", core=0, far=0, near=0, then=1)
    move("first", core=0, far=0, near=0, then=0)
    move("near", far=0, **end)
    move("far", near=0, **end)
    then(far=0, near=0)
    return moves


def solution(mesh):
    placed = (P(AXES, None), P(AXES, None), P(AXES))

    return jax.shard_map(
        per_device,
        mesh=mesh,
        in_specs=placed,
        out_specs=(P(AXES, None), P(AXES)),
        check_vma=False,
    )
```
